16 devices in a mesh: ep: 2 (over z), fsdp: 8 (over y, x, core).
Axes of the slice: x: 2, y: 2, z: 2, core: 2. Of those that a mesh axis runs over, the one named last changes fastest.
Arguments:
- x_in: bfloat16 [64, 512, 768], P(('ep', 'fsdp'))
- grad_y: bfloat16 [64, 512, 768], P(('ep', 'fsdp'))
- w_q: bfloat16 [768, 12, 64], P(('ep', 'fsdp'))
- w_k: bfloat16 [768, 12, 64], P(('ep', 'fsdp'))
- w_v: bfloat16 [768, 12, 64], P(('ep', 'fsdp'))
- w_o: bfloat16 [12, 64, 768], P(None, None, ('ep', 'fsdp'))
- gamma_attn: bfloat16 [768], P(('ep', 'fsdp'))
- gamma_mlp: bfloat16 [768], P(('ep', 'fsdp'))
- w_router: float32 [768, 8], P(('ep', 'fsdp'))
- w1_shared: bfloat16 [768, 3072], P(('ep', 'fsdp'))
- w3_shared: bfloat16 [768, 3072], P(('ep', 'fsdp'))
- w2_shared: bfloat16 [3072, 768], P(None, ('ep', 'fsdp'))
- w1_expert: bfloat16 [8, 768, 3072], P('ep', 'fsdp')
- w3_expert: bfloat16 [8, 768, 3072], P('ep', 'fsdp')
- w2_expert: bfloat16 [8, 3072, 768], P('ep', 'fsdp')
- expert_ids: int32 [64, 512], P(('ep', 'fsdp'))
Outputs:
- output 1: bfloat16 [64, 512, 768], P(('ep', 'fsdp'))
- output 2: bfloat16 [64, 512, 768], P(('ep', 'fsdp'))
- output 3: float32 [768, 12, 64], P(('ep', 'fsdp'))
- output 4: float32 [768, 12, 64], P(('ep', 'fsdp'))
- output 5: float32 [768, 12, 64], P(('ep', 'fsdp'))
- output 6: float32 [12, 64, 768], P(None, None, ('ep', 'fsdp'))
- output 7: float32 [768], P(('ep', 'fsdp'))
- output 8: float32 [768], P(('ep', 'fsdp'))
- output 9: float32 [768, 8], P(('ep', 'fsdp'))
- output 10: float32 [768, 3072], P(('ep', 'fsdp'))
- output 11: float32 [768, 3072], P(('ep', 'fsdp'))
- output 12: float32 [3072, 768], P(None, ('ep', 'fsdp'))
- output 13: float32 [8, 768, 3072], P('ep', 'fsdp')
- output 14: float32 [8, 768, 3072], P('ep', 'fsdp')
- output 15: float32 [8, 3072, 768], P('ep', 'fsdp')
All inputs are finite; a program needn't handle non-finite values.
Results may differ from the reference program's by a relative error of at most 0.02.
Values are sent between devices in bfloat16 or wider.
A program may use at most 1 GiB of HBM per device.

```python
import numpy as np
import jax
import jax.numpy as jnp
from jax import lax

DEVICES = 16
BATCH_DEV = 4
SEQ = 512
D = 768
HEADS = 12
KV_HEADS = 12
HEAD = 64
EXPERTS = 8
FF = 3072
FF_SH = 3072

BATCH_ALL = DEVICES * BATCH_DEV
TOKENS_DEV = BATCH_DEV * SEQ
CAPACITY = 2 * TOKENS_DEV // EXPERTS
Q_PER_KV = HEADS // KV_HEADS
Q_LEN = min(SEQ, 256)
EPS_NORM = 1e-5
EPS_QK = 1e-6
ROPE_BASE = 500000.0


def draw_expert_ids(root_key):
    hot_key, dev_key = jax.random.split(root_key)
    expert_order = jax.random.permutation(hot_key, EXPERTS)
    quarter = EXPERTS // 4
    per_expert = TOKENS_DEV // EXPERTS
    counts = np.array([2 * per_expert] * quarter + [per_expert] * quarter + [per_expert // 2] * (2 * quarter))
    base_ids = jnp.repeat(expert_order, counts, total_repeat_length=TOKENS_DEV)
    dev_keys = jax.random.split(dev_key, DEVICES)
    shuffled = jax.vmap(jax.random.permutation, in_axes=(0, None))(dev_keys, base_ids)
    return shuffled.reshape(BATCH_ALL, SEQ).astype(jnp.int32)


def setup_inputs(seed: int = 0) -> dict:
    sub_keys = jax.random.split(jax.random.key(seed), 16)

    def normal(draw_key, arr_shape, std_scale):
        return jax.random.normal(draw_key, arr_shape, jnp.float32) * std_scale

    x_in = normal(sub_keys[0], (BATCH_ALL, SEQ, D), 1.0).astype(jnp.bfloat16)
    grad_y = normal(sub_keys[1], (BATCH_ALL, SEQ, D), 1.0).astype(jnp.bfloat16)
    w_q = normal(sub_keys[2], (D, HEADS, HEAD), D ** -0.5).astype(jnp.bfloat16)
    w_k = normal(sub_keys[3], (D, KV_HEADS, HEAD), D ** -0.5).astype(jnp.bfloat16)
    w_v = normal(sub_keys[4], (D, KV_HEADS, HEAD), D ** -0.5).astype(jnp.bfloat16)
    w_o = normal(sub_keys[5], (HEADS, HEAD, D), 2.0 * (HEADS * HEAD) ** -0.5).astype(jnp.bfloat16)
    gamma_attn = (1.0 + 0.3 * normal(sub_keys[6], (D,), 1.0)).astype(jnp.bfloat16)
    gamma_mlp = (1.0 + 0.3 * normal(sub_keys[7], (D,), 1.0)).astype(jnp.bfloat16)
    w_router = normal(sub_keys[8], (D, EXPERTS), 0.6 * D ** -0.5)
    w1_shared = normal(sub_keys[9], (D, FF_SH), D ** -0.5).astype(jnp.bfloat16)
    w3_shared = normal(sub_keys[10], (D, FF_SH), D ** -0.5).astype(jnp.bfloat16)
    w2_shared = normal(sub_keys[11], (FF_SH, D), FF_SH ** -0.5).astype(jnp.bfloat16)
    w1_expert = normal(sub_keys[12], (EXPERTS, D, FF), 2.0 * D ** -0.5).astype(jnp.bfloat16)
    w3_expert = normal(sub_keys[13], (EXPERTS, D, FF), 2.0 * D ** -0.5).astype(jnp.bfloat16)
    w2_expert = normal(sub_keys[14], (EXPERTS, FF, D), FF ** -0.5).astype(jnp.bfloat16)
    expert_ids = draw_expert_ids(sub_keys[15])
    return {'x_in': x_in, 'grad_y': grad_y, 'w_q': w_q, 'w_k': w_k, 'w_v': w_v, 'w_o': w_o, 'gamma_attn': gamma_attn, 'gamma_mlp': gamma_mlp, 'w_router': w_router, 'w1_shared': w1_shared, 'w3_shared': w3_shared, 'w2_shared': w2_shared, 'w1_expert': w1_expert, 'w3_expert': w3_expert, 'w2_expert': w2_expert, 'expert_ids': expert_ids}


def rms_norm(tokens, gamma_vec):
    tok_f32 = tokens.astype(jnp.float32)
    inv_rms = lax.rsqrt(jnp.mean(tok_f32 * tok_f32, axis=-1, keepdims=True) + EPS_NORM)
    return (tok_f32 * inv_rms * gamma_vec.astype(jnp.float32)).astype(jnp.bfloat16)


def swiglu_act(up_gate, up_lin):
    return (jax.nn.silu(up_gate) * up_lin).astype(jnp.bfloat16)


def rope_tables():
    half_dim = HEAD // 2
    inv_freq = ROPE_BASE ** (-(jnp.arange(half_dim, dtype=jnp.float32) * 2.0 / HEAD))
    angles = jnp.arange(SEQ, dtype=jnp.float32)[:, None] * inv_freq[None, :]
    return jnp.cos(angles), jnp.sin(angles)


def rope_norm(heads_in, cos_tab, sin_tab):
    half_dim = heads_in.shape[-1] // 2
    head_vals = heads_in.astype(jnp.float32)
    first_half = head_vals[..., :half_dim]
    second_half = head_vals[..., half_dim:]
    cos_b = cos_tab[:, None, :]
    sin_b = sin_tab[:, None, :]
    rotated = jnp.concatenate([first_half * cos_b - second_half * sin_b, second_half * cos_b + first_half * sin_b], axis=-1)
    rotated = rotated * lax.rsqrt(jnp.mean(rotated * rotated, axis=-1, keepdims=True) + EPS_QK)
    return rotated.astype(jnp.bfloat16)


def seq_attention(seq_args):
    q_seq, k_seq, v_seq = seq_args
    cos_tab, sin_tab = rope_tables()
    q_rot = rope_norm(q_seq, cos_tab, sin_tab).reshape(SEQ // Q_LEN, Q_LEN, KV_HEADS, Q_PER_KV, HEAD)
    k_rot = rope_norm(k_seq, cos_tab, sin_tab).astype(jnp.float32)
    v_f32 = v_seq.astype(jnp.float32)
    key_pos = jnp.arange(SEQ)

    def one_block(blk_args):
        q_blk, blk_start = blk_args
        scores = jnp.einsum('qkgd,skd->kgqs', q_blk.astype(jnp.float32), k_rot) * HEAD ** -0.5
        causal = (blk_start + jnp.arange(Q_LEN))[:, None] >= key_pos[None, :]
        attn_probs = jax.nn.softmax(jnp.where(causal, scores, -1e30), axis=-1).astype(jnp.bfloat16)
        return jnp.einsum('kgqs,skd->qkgd', attn_probs.astype(jnp.float32), v_f32).astype(jnp.bfloat16)

    blocks_out = lax.map(jax.checkpoint(one_block), (q_rot, jnp.arange(SEQ // Q_LEN) * Q_LEN))
    return blocks_out.reshape(SEQ, HEADS, HEAD)


def layer_forward(x_in, w_q, w_k, w_v, w_o, gamma_attn, gamma_mlp, w_router, w1_shared, w3_shared, w2_shared, w1_expert, w3_expert, w2_expert, expert_ids):
    n_tok = BATCH_ALL * SEQ
    tokens = x_in.reshape(n_tok, D)
    normed1 = rms_norm(tokens, gamma_attn)
    normed1_f = normed1.astype(jnp.float32)
    q_proj = jnp.einsum('td,dhk->thk', normed1_f, w_q.astype(jnp.float32)).astype(jnp.bfloat16)
    k_proj = jnp.einsum('td,dhk->thk', normed1_f, w_k.astype(jnp.float32)).astype(jnp.bfloat16)
    v_proj = jnp.einsum('td,dhk->thk', normed1_f, w_v.astype(jnp.float32)).astype(jnp.bfloat16)
    attn_heads = lax.map(jax.checkpoint(seq_attention), (q_proj.reshape(BATCH_ALL, SEQ, HEADS, HEAD), k_proj.reshape(BATCH_ALL, SEQ, KV_HEADS, HEAD), v_proj.reshape(BATCH_ALL, SEQ, KV_HEADS, HEAD)))
    attn_out = jnp.einsum('thk,hkd->td', attn_heads.reshape(n_tok, HEADS, HEAD).astype(jnp.float32), w_o.astype(jnp.float32))
    hidden = (tokens.astype(jnp.float32) + attn_out).astype(jnp.bfloat16)
    normed2 = rms_norm(hidden, gamma_mlp)
    normed2_f = normed2.astype(jnp.float32)
    logits = jnp.dot(normed2_f, w_router)
    flat_ids = expert_ids.reshape(n_tok)
    gate_val = jax.nn.sigmoid(jnp.take_along_axis(logits, flat_ids[:, None], axis=1)[:, 0])
    routed_in = (gate_val[:, None] * normed2_f).astype(jnp.bfloat16)
    w1_f = w1_expert.astype(jnp.float32)
    w3_f = w3_expert.astype(jnp.float32)
    w2_f = w2_expert.astype(jnp.float32)

    def expert_block(blk_args):
        blk_in, blk_ids = blk_args
        onehot = blk_ids[:, None] == jnp.arange(EXPERTS)[None, :]
        running = jnp.cumsum(onehot.astype(jnp.int32), axis=0)
        dest_row = blk_ids * CAPACITY + jnp.sum(jnp.where(onehot, running, 0), axis=1) - 1
        buffer = jnp.zeros((EXPERTS * CAPACITY, D), jnp.bfloat16).at[dest_row].set(blk_in)
        buffer = buffer.reshape(EXPERTS, CAPACITY, D).astype(jnp.float32)
        up_gate = jnp.einsum('ecd,edf->ecf', buffer, w1_f)
        up_lin = jnp.einsum('ecd,edf->ecf', buffer, w3_f)
        act_rows = swiglu_act(up_gate, up_lin)
        down_rows = jnp.einsum('ecf,efd->ecd', act_rows.astype(jnp.float32), w2_f).astype(jnp.bfloat16)
        return down_rows.reshape(EXPERTS * CAPACITY, D)[dest_row]

    routed = lax.map(jax.checkpoint(expert_block), (routed_in.reshape(DEVICES, TOKENS_DEV, D), expert_ids.reshape(DEVICES, TOKENS_DEV))).reshape(n_tok, D)
    sh_gate = jnp.dot(normed2, w1_shared, preferred_element_type=jnp.float32)
    sh_lin = jnp.dot(normed2, w3_shared, preferred_element_type=jnp.float32)
    shared_out = jnp.dot(swiglu_act(sh_gate, sh_lin), w2_shared, preferred_element_type=jnp.float32)
    layer_out = (hidden.astype(jnp.float32) + routed.astype(jnp.float32) + shared_out).astype(jnp.bfloat16)
    return layer_out.reshape(BATCH_ALL, SEQ, D)


def reference(x_in, grad_y, w_q, w_k, w_v, w_o, gamma_attn, gamma_mlp, w_router, w1_shared, w3_shared, w2_shared, w1_expert, w3_expert, w2_expert, expert_ids):
    def forward(*params):
        return layer_forward(*params, expert_ids)

    layer_out, pullback = jax.vjp(forward, x_in, w_q, w_k, w_v, w_o, gamma_attn, gamma_mlp, w_router, w1_shared, w3_shared, w2_shared, w1_expert, w3_expert, w2_expert)
    grads = pullback(grad_y)
    return (layer_out, grads[0], grads[1].astype(jnp.float32), grads[2].astype(jnp.float32), grads[3].astype(jnp.float32), grads[4].astype(jnp.float32), grads[5].astype(jnp.float32), grads[6].astype(jnp.float32), grads[7].astype(jnp.float32), grads[8].astype(jnp.float32), grads[9].astype(jnp.float32), grads[10].astype(jnp.float32), grads[11].astype(jnp.float32), grads[12].astype(jnp.float32), grads[13].astype(jnp.float32))
```

```python
import functools
import math

import jax
import jax.numpy as jnp
from jax import lax
from jax.experimental import pallas as pl
from jax.experimental.pallas import tpu as pltpu
from jax.sharding import PartitionSpec as P


EPS_NORM = 1e-5
EPS_QK = 1e-6
ROPE_BASE = 500000.0
ALL_AXES = ('ep', 'fsdp')
PAIRS = [[0, 1], [2, 3], [4, 5], [6, 7]]
BF = jnp.bfloat16
F32 = jnp.float32
HEAD = 64
LANES = 128
Q_BLOCK = 256


def dot_nn(a, b):
    return lax.dot_general(a, b, (((1,), (0,)), ((), ())), preferred_element_type=F32)


def dot_nt(a, b):
    return lax.dot_general(a, b, (((1,), (1,)), ((), ())), preferred_element_type=F32)


def cost(flops, nbytes, trans=0):
    return pl.CostEstimate(flops=int(flops), bytes_accessed=int(nbytes), transcendentals=int(trans))


def params(*sem):
    return pltpu.CompilerParams(dimension_semantics=sem)


def head_tables(seq_len):
    half = HEAD // 2
    inv_freq = ROPE_BASE ** (-(jnp.arange(half, dtype=F32) * 2.0 / HEAD))
    angles = jnp.arange(seq_len, dtype=F32)[:, None] * inv_freq[None, :]
    cos, sin = jnp.cos(angles), jnp.sin(angles)
    cos_t = jnp.concatenate([cos, cos, cos, cos], axis=1)
    sin_t = jnp.concatenate([-sin, sin, -sin, sin], axis=1)
    return cos_t, sin_t


def swap_halves(x, low):
    return jnp.where(low, pltpu.roll(x, LANES - HEAD // 2, 1), pltpu.roll(x, HEAD // 2, 1))


def head_sum(x, first):
    a = jnp.sum(jnp.where(first, x, 0.0), axis=1, keepdims=True)
    b = jnp.sum(jnp.where(first, 0.0, x), axis=1, keepdims=True)
    return jnp.where(first, a, b)


def rope_unit(x, cos_t, sin_t, first, low):
    x = x.astype(F32)
    rot = x * cos_t + swap_halves(x, low) * sin_t
    inv = lax.rsqrt(head_sum(rot * rot, first) * (1.0 / HEAD) + EPS_QK)
    return rot, inv


def lane_masks(rows):
    lane = lax.broadcasted_iota(jnp.int32, (rows, LANES), 1)
    return lane < HEAD, (lane & (HEAD - 1)) < HEAD // 2


def causal_probs(k_rot, q_head, n_keys):
    scores = dot_nt(k_rot, q_head)
    e = jnp.exp2(scores * (HEAD ** -0.5 * math.log2(math.e)))
    n_q = q_head.shape[0]
    row = lax.broadcasted_iota(jnp.int32, (n_q, n_q), 0)
    col = lax.broadcasted_iota(jnp.int32, (n_q, n_q), 1)
    tail = jnp.where(row <= col, e[n_keys - n_q:], 0.0)
    e = tail if n_keys == n_q else jnp.concatenate([e[:n_keys - n_q], tail], axis=0)
    return e, 1.0 / jnp.sum(e, axis=0, keepdims=True)


def attn_fwd_kernel(q_ref, k_ref, v_ref, cos_ref, sin_ref, *rest):
    o_ref = rest[-1]
    seq = q_ref.shape[0]
    first, low = lane_masks(seq)
    cos_t, sin_t = cos_ref[...], sin_ref[...]
    q_rot, q_inv = rope_unit(q_ref[...], cos_t, sin_t, first, low)
    k_rot, k_inv = rope_unit(k_ref[...], cos_t, sin_t, first, low)
    q_unit = q_rot * q_inv
    k_unit = (k_rot * k_inv).astype(BF)
    v_t = v_ref[...].astype(F32).T.astype(BF)
    heads = [jnp.where(first, q_unit, 0.0).astype(BF), jnp.where(first, 0.0, q_unit).astype(BF)]
    for j in range(seq // Q_BLOCK):
        n_keys = (j + 1) * Q_BLOCK
        rows = slice(j * Q_BLOCK, n_keys)
        parts = []
        for h in range(2):
            e, inv_sum = causal_probs(k_unit[:n_keys], heads[h][rows], n_keys)
            probs = (e * inv_sum).astype(BF)
            out_t = dot_nn(v_t[:, :n_keys], probs)
            parts.append(out_t[h * HEAD:(h + 1) * HEAD])
        o_ref[rows, :] = jnp.concatenate(parts, axis=0).T.astype(BF)


def attn_bwd_kernel(q_ref, k_ref, v_ref, do_ref, cos_ref, sin_ref, *rest):
    dq_ref, dk_ref, dv_ref, dk_acc, dv_acc = rest[-5:]
    seq = q_ref.shape[0]
    first, low = lane_masks(seq)
    cos_t, sin_t = cos_ref[...], sin_ref[...]
    q_rot, q_inv = rope_unit(q_ref[...], cos_t, sin_t, first, low)
    k_rot, k_inv = rope_unit(k_ref[...], cos_t, sin_t, first, low)
    q_unit = q_rot * q_inv
    k_f32 = k_rot * k_inv
    k_unit = k_f32.astype(BF)
    k_t = k_f32.T.astype(BF)
    v = v_ref[...]
    d_out = do_ref[...].astype(F32)
    q_heads = [jnp.where(first, q_unit, 0.0).astype(BF), jnp.where(first, 0.0, q_unit).astype(BF)]
    do_heads = [jnp.where(first, d_out, 0.0).astype(BF), jnp.where(first, 0.0, d_out).astype(BF)]

    def unrope(d_unit, rot, inv, first, low, cos_t, sin_t):
        t = head_sum(d_unit * rot, first) * (1.0 / HEAD)
        d_rot = inv * d_unit - rot * (inv * inv * inv * t)
        return (d_rot * cos_t - swap_halves(d_rot, low) * sin_t).astype(BF)

    dk_acc[...] = jnp.zeros_like(dk_acc)
    dv_acc[...] = jnp.zeros_like(dv_acc)
    for j in range(seq // Q_BLOCK):
        n_keys = (j + 1) * Q_BLOCK
        rows = slice(j * Q_BLOCK, n_keys)
        parts = []
        for h in range(2):
            qh, doh = q_heads[h][rows], do_heads[h][rows]
            e, inv_sum = causal_probs(k_unit[:n_keys], qh, n_keys)
            probs = e * inv_sum
            d_probs = dot_nt(v[:n_keys], doh)
            delta = jnp.sum(probs * d_probs, axis=0, keepdims=True)
            d_scores = (probs * (d_probs - delta) * HEAD ** -0.5).astype(BF)
            dv_acc[:n_keys, :] += dot_nn(probs.astype(BF), doh)
            dk_acc[:n_keys, :] += dot_nn(d_scores, qh)
            dq_t = dot_nn(k_t[:, :n_keys], d_scores)
            parts.append(dq_t[h * HEAD:(h + 1) * HEAD])
        d_unit = jnp.concatenate(parts, axis=0).T
        dq_ref[rows, :] = unrope(d_unit, q_rot[rows], q_inv[rows], first[rows], low[rows], cos_t[rows], sin_t[rows])
    dk_ref[...] = unrope(dk_acc[...], k_rot, k_inv, first, low, cos_t, sin_t)
    dv_ref[...] = dv_acc[...].astype(BF)


def attn_call(kernel, arrays, offsets, tables, outs, n_out, lo, hi, seq, width, scratch, flops):
    n_tok = arrays[0].shape[0]
    groups = width // LANES
    block = lambda off: pl.BlockSpec((seq, LANES), lambda b, g: (b + lo, g + off))
    table = pl.BlockSpec((seq, LANES), lambda b, g: (0, 0))
    n_in = len(arrays) + 2
    rows = (hi - lo) * seq
    return pl.pallas_call(
        kernel,
        grid=(hi - lo, groups),
        in_specs=[block(off) for off in offsets] + [table, table] + [pl.BlockSpec(memory_space=pl.ANY)] * len(outs),
        out_specs=[block(0)] * n_out,
        out_shape=[jax.ShapeDtypeStruct((n_tok, width), BF)] * n_out,
        scratch_shapes=scratch,
        input_output_aliases={n_in + i: i for i in range(len(outs))},
        compiler_params=params('arbitrary', 'arbitrary'),
        cost_estimate=cost(flops * rows * seq * width, 2 * (len(arrays) + n_out) * rows * width),
    )(*arrays, *tables, *outs)


def attn_fwd(qkv, tables, seq, outs, lo, hi):
    width = qkv.shape[1] // 3
    groups = width // LANES
    return attn_call(attn_fwd_kernel, [qkv] * 3, [0, groups, 2 * groups], tables, outs, 1, lo, hi, seq, width, [], 20)


def attn_bwd(qkv, d_out, tables, seq, outs, lo, hi):
    width = d_out.shape[1]
    groups = width // LANES
    scratch = [pltpu.VMEM((seq, LANES), F32)] * 2
    return attn_call(attn_bwd_kernel, [qkv] * 3 + [d_out], [0, groups, 2 * groups, 0], tables, outs, 3, lo, hi, seq, width, scratch, 50)


def join_halves(ref, out):
    _, n, rows, _ = ref.shape
    for s in range(n):
        for h in range(2):
            lo = (2 * s + h) * rows
            out[lo:lo + rows, :] = ref[h, s]


def swiglu_kernel(chunk, split, x_ref, dy_ref, w1_ref, w3_ref, w2_ref, act_ref, dg_ref, dl_ref, *joined):
    if split:
        @pl.when(pl.program_id(1) == 0)
        def _():
            for ref, out in zip((w1_ref, w3_ref, w2_ref), joined):
                join_halves(ref, out)

        w1_ref, w3_ref, w2_ref = joined
    down = dot_nt if split else dot_nn
    for c in range(x_ref.shape[0] // chunk):
        rows = slice(c * chunk, (c + 1) * chunk)
        x = x_ref[rows, :]
        gate = dot_nn(x, w1_ref[...])
        lin = dot_nn(x, w3_ref[...])
        d_act = down(dy_ref[rows, :], w2_ref[...]).astype(BF).astype(F32)
        sig = jax.nn.sigmoid(gate)
        silu = gate * sig
        act_ref[rows, :] = (silu * lin).astype(BF)
        dl_ref[rows, :] = (d_act * silu).astype(BF)
        dg_ref[rows, :] = (d_act * lin * (sig * (1.0 + gate * (1.0 - sig)))).astype(BF)


def swiglu(x, d_y, weights, width, split, tm=1024, fb=768, chunk=1024):
    n_tok, dim = x.shape
    tok = pl.BlockSpec((tm, dim), lambda f, t: (t, 0))
    if split:
        up = [pl.BlockSpec(w.shape[:3] + (fb,), lambda f, t: (0, 0, 0, f)) for w in weights[:2]]
        part = weights[2].shape[2]
        w_specs = up + [pl.BlockSpec((2, fb // (2 * part), part, dim), lambda f, t: (0, f, 0, 0))]
    else:
        w_specs = [pl.BlockSpec((dim, fb), lambda f, t, off=i * width // fb: (0, f + off)) for i in range(3)]
        weights = [weights] * 3
    out = pl.BlockSpec((tm, fb), lambda f, t: (t, f))
    return pl.pallas_call(
        functools.partial(swiglu_kernel, chunk, split),
        grid=(width // fb, n_tok // tm),
        in_specs=[tok, tok] + w_specs,
        out_specs=[out] * 3,
        out_shape=[jax.ShapeDtypeStruct((n_tok, width), BF)] * 3,
        scratch_shapes=[pltpu.VMEM((dim, fb), BF)] * 2 + [pltpu.VMEM((fb, dim), BF)] if split else [],
        compiler_params=params('arbitrary', 'arbitrary'),
        cost_estimate=cost(6 * n_tok * dim * width, 6 * n_tok * width + 8 * n_tok * dim + 6 * dim * width, 2 * n_tok * width),
    )(x, d_y, *weights)


def mm_kernel(modes, n_extra, combine, split, *refs):
    n = len(modes)
    out = refs[2 * n + n_extra]
    b_refs = refs[1:2 * n:2]
    if split:
        joined = refs[2 * n + n_extra + 1:]

        @pl.when(pl.program_id(0) == 0)
        def _():
            for ref, whole in zip(b_refs, joined):
                join_halves(ref, whole)

        b_refs = joined
    acc = None
    for i, transposed in enumerate(modes):
        part = (dot_nt if transposed else dot_nn)(refs[2 * i][...], b_refs[i][...])
        acc = part if acc is None else acc + part
    extra = [r[...] for r in refs[2 * n:2 * n + n_extra]]
    out[...] = (combine(acc, *extra) if combine is not None else acc).astype(out.dtype)


def row_matmul(pairs, out_dim, out_dtype, extra=(), combine=None, split=False, tm=512):
    n_tok = pairs[0][0].shape[0]
    in_specs, args, scratch, flops, nbytes = [], [], [], 0, 0
    for a, b, transposed, off in pairs:
        k = a.shape[1]
        in_specs.append(pl.BlockSpec((tm, k), lambda t: (t, 0)))
        shape = (out_dim, k) if transposed else (k, out_dim)
        if split:
            scratch.append(pltpu.VMEM(shape, BF))
            in_specs.append(pl.BlockSpec(b.shape, lambda t: (0, 0, 0, 0), pipeline_mode=pl.Buffered(1)))
        else:
            in_specs.append(pl.BlockSpec(shape, lambda t, i=off // shape[1]: (0, i), pipeline_mode=pl.Buffered(1)))
        args += [a, b]
        flops += 2 * n_tok * k * out_dim
        nbytes += 2 * n_tok * k + 2 * k * out_dim
    for e in extra:
        in_specs.append(pl.BlockSpec((tm, out_dim), lambda t: (t, 0)))
        args.append(e)
        nbytes += e.size * e.dtype.itemsize
    return pl.pallas_call(
        functools.partial(mm_kernel, [p[2] for p in pairs], len(extra), combine, split),
        grid=(n_tok // tm,),
        in_specs=in_specs,
        out_specs=pl.BlockSpec((tm, out_dim), lambda t: (t, 0)),
        out_shape=jax.ShapeDtypeStruct((n_tok, out_dim), out_dtype),
        scratch_shapes=scratch,
        compiler_params=params('arbitrary'),
        cost_estimate=cost(flops, nbytes + n_tok * out_dim * jnp.dtype(out_dtype).itemsize),
    )(*args)


def copy_kernel(src, dst):
    dst[...] = src[...]


def copy_out(x):
    rows, cols = x.shape
    block = pl.BlockSpec((rows // 8, cols), lambda i: (i, 0))
    return pl.pallas_call(
        copy_kernel,
        grid=(8,),
        in_specs=[block],
        out_specs=block,
        out_shape=jax.ShapeDtypeStruct(x.shape, x.dtype),
        compiler_params=params('arbitrary'),
        cost_estimate=cost(rows * cols, 8 * rows * cols),
    )(x)


def grad_kernel(spans, layout, *refs):
    n_a = len(spans)
    n_b = sum(len(s) for s in spans)
    a_refs, b_refs = refs[:n_a], refs[n_a:n_a + n_b]
    out_ref, a_t = refs[n_a + n_b], refs[n_a + n_b + 1]
    j = pl.program_id(0)
    i = 0
    for a, group in enumerate(spans):
        @pl.when(j == group[0][0])
        def _(a=a):
            a_t[...] = a_refs[a][...].T

        for lo, hi in group:
            @pl.when((j >= lo) & (j < hi))
            def _(i=i):
                g = dot_nn(a_t[...], b_refs[i][...])
                if layout == 'plain':
                    out_ref[...] = g
                elif layout == 'rows':
                    n_s, part = out_ref.shape[1], out_ref.shape[2]
                    for s in range(n_s):
                        for h in range(2):
                            lo_row = (s * 2 + h) * part
                            out_ref[h, s] = g[lo_row:lo_row + part]
                else:
                    g = g.T
                    n_s, part = out_ref.shape[1], out_ref.shape[2]
                    for s in range(n_s):
                        for h in range(2):
                            lo_row = (s * 2 + h) * part
                            out_ref[h, s] = g[lo_row:lo_row + part]

            i += 1


def weight_grads(groups, layout='plain', nb=768, n_dest=8):
    n_tok, dim = groups[0][0].shape
    spans, a_list, b_list, b_specs, lo = [], [], [], [], 0
    for a, bs in groups:
        a_list.append(a)
        span = []
        for b in bs:
            n = b.shape[1] // nb
            span.append((lo, lo + n))
            b_specs.append(pl.BlockSpec((n_tok, nb), lambda j, lo=lo, n=n: (0, jnp.clip(j - lo, 0, n - 1))))
            b_list.append(b)
            lo += n
        spans.append(span)
    total = lo * nb
    if layout == 'plain':
        out_spec = pl.BlockSpec((dim, nb), lambda j: (0, j))
        out_shape = (dim, total)
    elif layout == 'rows':
        out_spec = pl.BlockSpec((2, n_dest, dim // (2 * n_dest), nb), lambda j: (0, 0, 0, j))
        out_shape = (2, n_dest, dim // (2 * n_dest), total)
    else:
        part = total // (2 * n_dest)
        out_spec = pl.BlockSpec((2, nb // (2 * part), part, dim), lambda j: (0, j, 0, 0))
        out_shape = (2, n_dest, part, dim)
    return pl.pallas_call(
        functools.partial(grad_kernel, spans, layout),
        grid=(lo,),
        in_specs=[pl.BlockSpec((n_tok, dim), lambda j: (0, 0), pipeline_mode=pl.Buffered(1))] * len(a_list) + b_specs,
        out_specs=out_spec,
        out_shape=jax.ShapeDtypeStruct(out_shape, F32),
        scratch_shapes=[pltpu.VMEM((dim, n_tok), BF)],
        compiler_params=params('arbitrary'),
        cost_estimate=cost(2 * n_tok * dim * total, 2 * n_tok * (dim + total) + 4 * dim * total),
    )(*a_list, *b_list)


def rms_scale(tokens):
    return lax.rsqrt(jnp.mean(tokens * tokens, axis=-1, keepdims=True) + EPS_NORM)


def rms_back(d_norm, tokens, inv_rms, gamma_vec):
    scaled = d_norm * gamma_vec
    dot = jnp.mean(scaled * tokens, axis=-1, keepdims=True)
    d_tokens = inv_rms * scaled - tokens * (inv_rms * inv_rms * inv_rms * dot)
    d_gamma = jnp.sum(d_norm * (tokens * inv_rms), axis=0)
    return d_tokens, d_gamma


def route_slots(flat_ids, n_experts, capacity):
    onehot = flat_ids[:, None] == jnp.arange(n_experts)[None, :]
    running = jnp.cumsum(onehot.astype(jnp.int32), axis=0)
    slot_idx = jnp.sum(jnp.where(onehot, running, 0), axis=1) - 1
    return onehot, flat_ids * capacity + slot_idx


def exchange(x, axes):
    return lax.all_to_all(x, axes, 0, 0, tiled=True)


def to_expert(rows, n_dev):
    n_slots, dim = rows.shape
    return exchange(rows.reshape(n_dev, n_slots // n_dev, dim), ALL_AXES).reshape(n_slots, dim)


def fetch_expert(w_block, n_fsdp):
    e_local, rows, cols = w_block.shape
    mine = exchange(w_block.reshape(n_fsdp, rows * e_local // n_fsdp, cols), 'fsdp')
    return lax.all_gather(mine, 'fsdp', axis=0, tiled=False, axis_index_groups=PAIRS)


def return_grad(grad, e_local):
    n_fsdp = grad.shape[1]
    summed = lax.psum_scatter(grad, 'fsdp', scatter_dimension=0, tiled=False, axis_index_groups=PAIRS)
    back = exchange(summed, 'fsdp')
    rows, cols = summed.shape[1:]
    return copy_out(back.reshape(n_fsdp * rows, cols)).reshape(e_local, n_fsdp // e_local * rows, cols)


def spread(rows, dest_row, n_slots):
    return jnp.zeros((n_slots, rows.shape[1]), BF).at[dest_row].set(rows, unique_indices=True, mode='promise_in_bounds')


def device_step(n_dev, n_fsdp, x_in, grad_y, w_q, w_k, w_v, w_o, gamma_attn, gamma_mlp, w_router, w1_shared, w3_shared, w2_shared, w1_expert, w3_expert, w2_expert, expert_ids):
    n_batch, seq_len, dim = x_in.shape
    n_tok = n_batch * seq_len
    n_heads = w_q.shape[1]
    width = n_heads * HEAD
    n_experts = w_router.shape[1]
    e_local = w1_expert.shape[0]
    ff = w1_shared.shape[1]
    ff_e = w1_expert.shape[2]
    shard = w_q.shape[0]
    capacity = 2 * n_tok // n_experts
    n_slots = n_experts * capacity

    small = jnp.concatenate([w_router, gamma_attn.astype(F32)[:, None], gamma_mlp.astype(F32)[:, None]], axis=1)
    small = exchange(jnp.broadcast_to(small.reshape(1, 1, small.size), (n_dev, 1, small.size)), ALL_AXES).reshape(dim, n_experts + 2)
    wr, ga, gm = small[:, :n_experts], small[:, n_experts], small[:, n_experts + 1]
    w_attn = jnp.concatenate([w_q.reshape(shard, width), w_k.reshape(shard, width), w_v.reshape(shard, width), w_o.reshape(width, shard).T], axis=1)
    w_attn = lax.all_gather(w_attn, ALL_AXES, axis=0, tiled=True)
    w_sh = jnp.concatenate([w1_shared, w3_shared, w2_shared.T], axis=1)
    w_sh = lax.all_gather(w_sh, ALL_AXES, axis=0, tiled=True)
    w1e, w3e, w2e = (fetch_expert(w, n_fsdp) for w in (w1_expert, w3_expert, w2_expert))

    onehot, dest_row = route_slots(expert_ids.reshape(n_tok), n_experts, capacity)
    d_out = grad_y.reshape(n_tok, dim)
    d_down = to_expert(spread(d_out, dest_row, n_slots), n_dev)

    tables = head_tables(seq_len)
    tokens = x_in.reshape(n_tok, dim)
    tok_f = tokens.astype(F32)
    inv1 = rms_scale(tok_f)
    normed1 = (tok_f * inv1 * ga).astype(BF)
    qkv = jnp.dot(normed1, w_attn[:, :3 * width], preferred_element_type=F32).astype(BF)
    attn = []
    for b in range(n_batch):
        attn = attn_fwd(qkv, tables, seq_len, attn, b, b + 1)
    attn = attn[0]
    attn_out = dot_nt(attn, w_attn[:, 3 * width:])
    hidden = (tok_f + attn_out).astype(BF)
    hid_f = hidden.astype(F32)
    inv2 = rms_scale(hid_f)
    normed2 = (hid_f * inv2 * gm).astype(BF)
    normed2_f = normed2.astype(F32)
    logits = jnp.dot(normed2, wr, preferred_element_type=F32, precision=lax.Precision.HIGHEST)
    gate_val = jax.nn.sigmoid(jnp.sum(jnp.where(onehot, logits, 0.0), axis=1))
    routed_in = (gate_val[:, None] * normed2_f).astype(BF)
    rows = to_expert(spread(routed_in, dest_row, n_slots), n_dev)

    act_s, dg_s, dl_s = swiglu(normed2, d_out, w_sh, ff, False)
    base = row_matmul([(act_s, w_sh, True, 2 * ff)], dim, F32, extra=(hidden,), combine=lambda acc, h: h.astype(F32) + acc)
    d_n2_shared = row_matmul([(dg_s, w_sh, True, 0), (dl_s, w_sh, True, ff)], dim, F32)
    g_sh = weight_grads([(normed2, [dg_s, dl_s]), (d_out, [act_s])])
    g_sh = lax.psum_scatter(g_sh, ALL_AXES, scatter_dimension=0, tiled=True)

    act_e, dg_e, dl_e = swiglu(rows, d_down, (w1e, w3e, w2e), ff_e, True)
    d_rows = row_matmul([(dg_e, w1e, True, 0), (dl_e, w3e, True, 0)], dim, BF, split=True)
    d_back = to_expert(d_rows, n_dev)
    down = row_matmul([(act_e, w2e, False, 0)], dim, BF, split=True)
    back = to_expert(down, n_dev)
    g_w2e = return_grad(weight_grads([(d_down, [act_e])], 'cols', n_dest=n_fsdp), e_local)
    g_w1e = return_grad(weight_grads([(rows, [dg_e])], 'rows', n_dest=n_fsdp), e_local)
    g_w3e = return_grad(weight_grads([(rows, [dl_e])], 'rows', n_dest=n_fsdp), e_local)
    routed = back.at[dest_row].get(mode='promise_in_bounds').astype(F32)
    layer_out = (base + routed).astype(BF)

    d_routed = d_back.at[dest_row].get(mode='promise_in_bounds').astype(F32)
    d_gate = jnp.sum(d_routed * normed2_f, axis=1) * gate_val * (1.0 - gate_val)
    d_logits = jnp.where(onehot, d_gate[:, None], 0.0)
    g_wr = jnp.einsum('td,te->de', normed2_f, d_logits, precision=lax.Precision.HIGHEST)
    d_n2 = d_n2_shared + gate_val[:, None] * d_routed + jnp.einsum('te,de->td', d_logits, wr, precision=lax.Precision.HIGHEST)
    d_hid, g_gm = rms_back(d_n2.astype(BF).astype(F32), hid_f, inv2, gm)
    d_hidden = (d_out.astype(F32) + d_hid.astype(BF).astype(F32)).astype(BF)

    d_attn = jnp.dot(d_hidden, w_attn[:, 3 * width:], preferred_element_type=F32).astype(BF)
    d_qkv = []
    for b in range(n_batch):
        d_qkv = attn_bwd(qkv, d_attn, tables, seq_len, d_qkv, b, b + 1)
    d_q, d_k, d_v = d_qkv
    g_attn = weight_grads([(normed1, [d_q, d_k, d_v]), (d_hidden, [attn])])
    g_attn = lax.psum_scatter(g_attn, ALL_AXES, scatter_dimension=0, tiled=True)
    d_n1 = row_matmul([(d_q, w_attn, True, 0), (d_k, w_attn, True, width), (d_v, w_attn, True, 2 * width)], dim, F32)
    d_tok, g_ga = rms_back(d_n1.astype(BF).astype(F32), tok_f, inv1, ga)
    d_x = (d_hidden.astype(F32) + d_tok.astype(BF).astype(F32)).astype(BF)

    tiny = jnp.concatenate([g_wr, g_ga[:, None], g_gm[:, None]], axis=1).reshape(n_dev, shard, n_experts + 2)
    tiny = jnp.sum(exchange(tiny, ALL_AXES), axis=0)

    g_q, g_k, g_v = (g_attn[:, i * width:(i + 1) * width].reshape(shard, n_heads, HEAD) for i in range(3))
    g_o = g_attn[:, 3 * width:].T.reshape(n_heads, HEAD, shard)
    return (layer_out.reshape(x_in.shape), d_x.reshape(x_in.shape), g_q, g_k, g_v, g_o, tiny[:, n_experts], tiny[:, n_experts + 1], tiny[:, :n_experts],
            g_sh[:, :ff], g_sh[:, ff:2 * ff], g_sh[:, 2 * ff:].T, g_w1e, g_w3e, g_w2e)


def solution(mesh):
    tok_spec = P(ALL_AXES, None, None)
    mat_spec = P(ALL_AXES, None)
    vec_spec = P(ALL_AXES)
    wo_spec = P(None, None, ALL_AXES)
    w2s_spec = P(None, ALL_AXES)
    exp_spec = P('ep', 'fsdp', None)
    in_specs = (tok_spec, tok_spec, tok_spec, tok_spec, tok_spec, wo_spec, vec_spec, vec_spec, mat_spec, mat_spec, mat_spec, w2s_spec, exp_spec, exp_spec, exp_spec, mat_spec)
    out_specs = (tok_spec, tok_spec, tok_spec, tok_spec, tok_spec, wo_spec, vec_spec, vec_spec, mat_spec, mat_spec, mat_spec, w2s_spec, exp_spec, exp_spec, exp_spec)

    def step(*args):
        return device_step(mesh.size, mesh.shape['fsdp'], *args)

    return jax.shard_map(step, mesh=mesh, in_specs=in_specs, out_specs=out_specs, check_vma=False)
```
